32 devices in a mesh: dp: 8 (over z, y), owner: 4 (over x, core).
Axes of the slice: x: 2, y: 2, z: 4, core: 2. Of those that a mesh axis runs over, the one named last changes fastest.
Arguments:
- gradients: bfloat16 [8, 4, 512, 512], P('dp', 'owner'), may hold values from -600 to 600
- block_layer: int32 [4], P('owner'), may hold values from 0 to 3
Outputs:
- update: bfloat16 [4, 512, 512], P('owner', 'dp')
The draws below stay inside these ranges and needn't reach their ends.
All inputs are finite; a program needn't handle non-finite values.
Results may differ from the reference program's by a relative error of at most 0.0062.
Values may be sent and summed in bfloat16 or wider, within the bound.
A program may use at most 64 MiB of HBM per device.

```python
import math
import jax
import jax.numpy as jnp
from jax import lax

B = 512
LAYERS = 4
ITERS = 3
NBLK = 4
N_DP = 8


def draw_gradients(key, part):
    first_key = jax.random.fold_in(jax.random.fold_in(key, 11), 0)
    third_key = jax.random.fold_in(jax.random.fold_in(key, 11), 2)
    fourth_key = jax.random.fold_in(jax.random.fold_in(key, 11), 3)
    fifth_key = jax.random.fold_in(jax.random.fold_in(key, 11), 4)
    scales = jnp.exp(jax.random.uniform(first_key, (N_DP, NBLK, 1, 1), jnp.float32, 0.0, math.log(10.0)))
    heavy = jax.random.randint(fourth_key, (1, NBLK, 1, 1), 0, N_DP)
    replica_ids = jnp.arange(N_DP, dtype=jnp.int32)[:, None, None, None]
    scales = jnp.where(replica_ids == heavy, 25.0, scales)
    row_place = jnp.arange(B, dtype=jnp.float32)[None, None, :, None] / float(B - 1)
    jitter = jnp.exp(jax.random.uniform(fifth_key, (1, NBLK, B, 1), jnp.float32, math.log(0.8), math.log(1.25)))
    ramp = jnp.exp(0.5 * math.log(10.0) * row_place) * jitter
    values = jnp.clip(jax.random.normal(third_key, (N_DP, NBLK, B, B), jnp.float32), -6.0, 6.0)
    return (scales * ramp * values).astype(jnp.bfloat16)


def with_ends(array, stream_key, low, high):
    extent = array.shape
    place = [jax.random.randint(jax.random.fold_in(stream_key, axis), (), 0, extent[axis]) for axis in range(len(extent))]
    array = array.at[tuple(place)].set(low)
    longest = extent.index(max(extent))
    place[longest] = (place[longest] + 1) % extent[longest]
    return array.at[tuple(place)].set(high)


def setup_inputs(seed: int = 0) -> dict:
    arg_keys = jax.random.split(jax.random.key(seed), 3)
    return {
        "gradients": draw_gradients(jax.random.fold_in(arg_keys[2], 71), 0),
        "block_layer": with_ends(jax.random.randint(arg_keys[1], (NBLK,), 0, LAYERS), jax.random.fold_in(arg_keys[1], 1), 0, LAYERS - 1).astype(jnp.int32),
    }


def inverse_root(statistic):
    size_b = statistic.shape[0]
    identity = jnp.eye(size_b, dtype=jnp.float32)
    ridge_term = 0.01 * jnp.trace(statistic) / size_b + 1e-06
    shifted = statistic + ridge_term * identity
    scaling = jnp.sqrt(jnp.sum(shifted * shifted))
    current = shifted / scaling
    inverse = identity
    for step_number in range(ITERS):
        factor = (5.0 * identity - current) / 4.0
        if step_number == 0:
            inverse = scaling ** (-0.25) * factor
        else:
            inverse = jnp.dot(inverse, factor, precision=lax.Precision.HIGHEST)
        if step_number + 1 < ITERS:
            square = jnp.dot(factor, factor, precision=lax.Precision.HIGHEST)
            fourth = jnp.dot(square, square, precision=lax.Precision.HIGHEST)
            current = jnp.dot(fourth, current, precision=lax.Precision.HIGHEST)
    return inverse

def one_block(block_grads):
    widened = block_grads.astype(jnp.float32)
    left_sum = jnp.einsum('dij,dkj->ik', widened, widened, precision=lax.Precision.HIGHEST)
    right_sum = jnp.einsum('dji,djk->ik', widened, widened, precision=lax.Precision.HIGHEST)
    left_root = lax.optimization_barrier(inverse_root(left_sum).astype(jnp.bfloat16)).astype(jnp.float32)
    right_root = lax.optimization_barrier(inverse_root(right_sum).astype(jnp.bfloat16)).astype(jnp.float32)
    total_sum = lax.optimization_barrier(jnp.sum(widened, axis=0))
    middle = jnp.dot(left_root, total_sum, precision=lax.Precision.HIGHEST)
    return jnp.dot(middle, right_root, precision=lax.Precision.HIGHEST) / N_DP

def reference(gradients, block_layer):
    precond = lax.map(one_block, jnp.swapaxes(gradients, 0, 1))
    energy = lax.optimization_barrier(jnp.sum(precond * precond, axis=(1, 2)))
    selector = (block_layer[:, None] == jnp.arange(LAYERS, dtype=jnp.int32)[None, :]).astype(jnp.float32)
    layer_energy = lax.optimization_barrier(jnp.sum(selector * energy[:, None], axis=0))
    layer_count = lax.optimization_barrier(jnp.sum(selector, axis=0)) * float(B * B)
    block_mean = lax.optimization_barrier(jnp.sum(selector * layer_energy[None, :], axis=1)) / lax.optimization_barrier(jnp.sum(selector * layer_count[None, :], axis=1))
    return (precond * lax.rsqrt(block_mean + 1e-06)[:, None, None]).astype(jnp.bfloat16)
```

```python
import functools

import jax
import jax.numpy as jnp
from jax import lax
from jax.experimental import pallas as pl
from jax.experimental.pallas import tpu as pltpu
from jax.sharding import PartitionSpec as P

ITERS = 3
TILE = 128
EXTRA = 16
GRAD_ORDERS = (None, None)
PROGRAM = (
    "+L gR +R "
    "L +0 R +1 Lx Rx 0 1 L l l l 0x l 1x R r r r r 0 1"
)
BF16 = jnp.bfloat16
F32 = jnp.float32
MESH = pl.DeviceIdType.MESH


def mm(a, b):
    return jnp.dot(a.astype(BF16), b.astype(BF16), preferred_element_type=F32)


def iotas(rows, cols):
    return (
        lax.broadcasted_iota(jnp.int32, (rows, cols), 0),
        lax.broadcasted_iota(jnp.int32, (rows, cols), 1),
    )


def off_tiles(size_b):
    t = size_b // TILE
    return [(i, j) for i in range(t) for j in range(i + 1, t)]


def tile(array, i, j):
    return array[i * TILE:(i + 1) * TILE, j * TILE:(j + 1) * TILE]


def place(n, per_quarter):
    row = n % per_quarter * TILE
    return n // per_quarter, slice(row, row + TILE)


def pack(gram, acc_ref, size_b):
    t = size_b // TILE
    per_quarter = t * t // 8
    row, col = iotas(TILE, TILE)
    sub, _ = iotas(EXTRA, TILE)
    extra = jnp.zeros((EXTRA, TILE), F32)
    n = 0
    for d in range(0, t, 2):
        second = tile(gram, d + 1, d + 1)
        q, rows = place(n, per_quarter)
        acc_ref[q, rows, :] = jnp.where(row <= col, tile(gram, d, d), second).astype(BF16)
        diagonal = jnp.sum(jnp.where(row == col, second, 0.0), axis=0, keepdims=True)
        extra = jnp.where(sub == d // 2, diagonal, extra)
        n += 1
    for i, j in off_tiles(size_b):
        q, rows = place(n, per_quarter)
        acc_ref[q, rows, :] = tile(gram, i, j).astype(BF16)
        n += 1
    for q in range(4):
        value = extra if q == 0 else jnp.zeros((EXTRA, TILE), F32)
        acc_ref[q, per_quarter * TILE:, :] = value.astype(BF16)


def unpack(gath_ref, stat_ref, size_b):
    t = size_b // TILE
    per_quarter = t * t // 8
    row, col = iotas(TILE, TILE)
    extra = gath_ref[0, per_quarter * TILE:, :].astype(F32)
    n = 0
    for d in range(0, t, 2):
        q, rows = place(n, per_quarter)
        both = gath_ref[q, rows, :].astype(F32)
        turned = both.T
        first = jnp.where(row <= col, both, turned)
        second = jnp.where(row > col, both, turned)
        second = jnp.where(row == col, extra[d // 2:d // 2 + 1, :], second)
        for k, block in ((d, first), (d + 1, second)):
            stat_ref[k * TILE:(k + 1) * TILE, k * TILE:(k + 1) * TILE] = block
        n += 1
    for i, j in off_tiles(size_b):
        q, rows = place(n, per_quarter)
        block = gath_ref[q, rows, :].astype(F32)
        stat_ref[i * TILE:(i + 1) * TILE, j * TILE:(j + 1) * TILE] = block
        stat_ref[j * TILE:(j + 1) * TILE, i * TILE:(i + 1) * TILE] = block.T
        n += 1


def solver(gath_ref, stat_ref, size_b, result):
    unpack(gath_ref, stat_ref, size_b)
    row, col = iotas(size_b, size_b)
    diag = row == col
    stat = stat_ref[...]
    trace = jnp.sum(jnp.where(diag, stat, 0.0), keepdims=True)
    ridge = 0.01 * trace / size_b + 1e-06
    shifted = stat + jnp.where(diag, ridge, 0.0)
    norm2 = jnp.sum(shifted * shifted, keepdims=True)
    m = shifted * lax.rsqrt(norm2)
    a, y = 1.25, -0.25 * m
    for step in range(1, ITERS):
        yield
        square = mm(m, m)
        once = (25.0 * m - 10.0 * square + mm(m, square)) * 0.0625
        yield
        m = 1.5625 * once + mm((square - 10.0 * m) * 0.0625, once)
        if step + 1 < ITERS:
            y = 1.25 * y - (0.25 * a) * m - 0.25 * mm(y, m)
            a = 1.25 * a
    result["scale"] = lax.rsqrt(jnp.sqrt(jnp.sqrt(norm2)))
    result["a"], result["y"], result["m"] = a, y, m


class Piece:
    def __init__(self, me, nb, order, src, land, forward, xsend, xland, gath, send, recv, target):
        self.me, self.nb, self.order = me, nb, order
        self.src, self.land, self.forward = src, land, forward
        self.xsend, self.xland, self.gath = xsend, xland, gath
        self.send, self.recv, self.target = send, recv, target
        self.mine = lax.rem(me, 4)
        self.flow = self.run()
        self.started = []

    def partner(self, mask):
        other = self.me
        for number in range(self.nb):
            if mask >> number & 1:
                other = other + (1 - 2 * (self.me // (1 << number) % 2)) * (1 << number)
        return other

    def copy(self, src, dst, slot, mask):
        copy = pltpu.make_async_remote_copy(
            src_ref=src,
            dst_ref=dst,
            send_sem=self.send.at[slot],
            recv_sem=self.recv.at[slot],
            device_id=self.target(self.partner(mask)),
            device_id_type=MESH,
        )
        copy.start()
        self.started.append(copy)
        return copy

    def run(self):
        low = lambda mask: lax.rem(self.partner(mask), 4)
        if self.order is None:
            copies = [
                self.copy(self.src(low(mask)), self.land.at[mask - 1], mask - 1, mask)
                for mask in (1, 2, 3)
            ]
            yield
            total = self.src(self.mine)[...].astype(F32)
            for n, copy in enumerate(copies):
                copy.wait_recv()
                total += self.land[n].astype(F32)
        else:
            first, second = (1 << bit for bit in self.order)
            onward = self.copy(self.src(low(3)), self.land.at[0], 0, first)
            stay = self.copy(self.src(low(first)), self.land.at[1], 1, first)
            yield
            onward.wait_recv()
            passing = self.src(low(second))[...].astype(F32) + self.land[0].astype(F32)
            self.forward[...] = passing.astype(BF16)
            last = self.copy(self.forward, self.land.at[2], 2, second)
            yield
            stay.wait_recv()
            total = self.src(self.mine)[...].astype(F32) + self.land[1].astype(F32)
            last.wait_recv()
            total += self.land[2].astype(F32)
        for n in range(self.nb - 2):
            self.xsend[n] = total.astype(BF16)
            copy = self.copy(self.xsend.at[n], self.xland.at[n], 6 + n, 4 << n)
            yield
            copy.wait_recv()
            total = self.xsend[n].astype(F32) + self.xland[n].astype(F32)
        self.gath(self.mine)[...] = total.astype(BF16)
        own = self.gath(self.mine)
        if self.order is None:
            copies = [self.copy(own, own, 2 + mask, mask) for mask in (1, 2, 3)]
            yield
            for copy in copies:
                copy.wait_recv()
        else:
            near = self.copy(own, own, 3, second)
            far = self.copy(own, own, 4, first)
            yield
            near.wait_recv()
            other = self.gath(low(second))
            rest = self.copy(other, other, 5, first)
            yield
            far.wait_recv()
            rest.wait_recv()

    def attend(self):
        next(self.flow, None)


def kernel(dp_count, owners, layer_ref, g_ref, out_ref, acc_s, gath_s, land_s, xsend_s,
           xland_s, gath_g, land_g, forward_g, xsend_g, xland_g, stats, whole_ref, e_src, e_buf,
           send, recv, e_send, e_recv):
    me = lax.axis_index("dp")
    own = lax.axis_index("owner")
    size_b = g_ref.shape[0]
    nb = dp_count.bit_length() - 1
    quarter = size_b // 4
    chunks = len(GRAD_ORDERS)
    width = size_b // chunks

    target = lambda partner: (partner, own)
    pieces = {}
    for n, name in enumerate("LR"):
        pieces[name] = Piece(
            me, nb, None, lambda q, n=n: acc_s.at[n, q], land_s.at[n], None, xsend_s.at[n],
            xland_s.at[n], lambda q, n=n: gath_s.at[n, q], send.at[n], recv.at[n], target,
        )
    for n, order in enumerate(GRAD_ORDERS):
        def block(ref, n=n):
            def at(q):
                rows = pl.ds(pl.multiple_of(q * quarter, quarter), quarter)
                return ref.at[rows, n * width:(n + 1) * width]
            return at
        pieces[str(n)] = Piece(
            me, nb, order, block(g_ref), land_g.at[n], forward_g.at[n], xsend_g.at[n],
            xland_g.at[n], block(gath_g), send.at[2 + n], recv.at[2 + n], target,
        )

    barrier = pltpu.get_barrier_semaphore()
    masks = [1, 2, 3] + [4 << n for n in range(nb - 2)]
    for mask in masks:
        peer = pieces["L"].partner(mask)
        pl.semaphore_signal(barrier, inc=1, device_id=(peer, own), device_id_type=MESH)
    for j in range(1, owners):
        pl.semaphore_signal(
            barrier, inc=1, device_id=(me, lax.rem(own + j, owners)), device_id_type=MESH
        )
    g = g_ref[...]
    pack(
        lax.dot_general(g, g, (((1,), (1,)), ((), ())), preferred_element_type=F32),
        acc_s.at[0], size_b,
    )
    pl.semaphore_wait(barrier, len(masks) + owners - 1)

    left, right = {}, {}
    solves = {
        "l": solver(gath_s.at[0], stats.at[0], size_b, left),
        "r": solver(gath_s.at[1], stats.at[1], size_b, right),
    }
    for token in PROGRAM.split():
        if token == "gR":
            pack(
                lax.dot_general(g, g, (((0,), (0,)), ((), ())), preferred_element_type=F32),
                acc_s.at[1], size_b,
            )
        elif token in solves:
            next(solves[token], None)
        elif token[-1] == "x":
            for _ in range(nb - 2):
                pieces[token[0]].attend()
        else:
            pieces[token[-1]].attend()
    for solve in solves.values():
        for _ in solve:
            pass

    grad = gath_g[...]
    y, m, a = left["y"], left["m"], left["a"]
    y = 1.25 * y - (0.25 * a) * m - 0.25 * mm(y, m)
    middle = left["scale"] * ((1.25 * a) * grad.astype(F32) + mm(y, grad))
    half = right["a"] * middle + mm(middle, right["y"])
    whole = (right["scale"] / dp_count) * (1.25 * half - 0.25 * mm(half, right["m"]))
    whole_ref[...] = whole
    energy = jnp.sum(whole * whole, keepdims=True)

    layer = layer_ref[0]
    sub, lane = iotas(*e_src.shape)
    mine = lane == layer
    value = jnp.where(sub == 0, energy, float(size_b * size_b))
    e_src[...] = jnp.where(mine, value, 0.0)
    copies = []
    for j in range(1, owners):
        copy = pltpu.make_async_remote_copy(
            src_ref=e_src,
            dst_ref=e_buf.at[j - 1],
            send_sem=e_send.at[j - 1],
            recv_sem=e_recv.at[j - 1],
            device_id=(me, lax.rem(own + j, owners)),
            device_id_type=MESH,
        )
        copy.start()
        copies.append(copy)
    for piece in pieces.values():
        for copy in piece.started:
            copy.wait_send()
    height = out_ref.shape[0]
    rows = whole_ref[pl.ds(pl.multiple_of(me * height, 16), height), :]
    totals = e_src[...]
    for j, copy in enumerate(copies):
        copy.wait()
        totals += e_buf[j]
    energies = jnp.sum(jnp.where(mine & (sub == 0), totals, 0.0), keepdims=True)
    counts = jnp.sum(jnp.where(mine & (sub == 1), totals, 0.0), keepdims=True)
    out_ref[...] = (rows * lax.rsqrt(energies / counts + 1e-06)).astype(BF16)


def per_device(dp_count, owners, gradients, block_layer):
    size_b = gradients.shape[-1]
    nb = dp_count.bit_length() - 1
    height = size_b // dp_count
    per_quarter = (size_b // TILE) ** 2 // 8 * TILE + EXTRA
    chunks = len(GRAD_ORDERS)
    part = (size_b // 4, size_b // chunks)
    out = pl.pallas_call(
        functools.partial(kernel, dp_count, owners),
        out_shape=jax.ShapeDtypeStruct((height, size_b), BF16),
        in_specs=[
            pl.BlockSpec(memory_space=pltpu.SMEM),
            pl.BlockSpec(memory_space=pltpu.VMEM),
        ],
        out_specs=pl.BlockSpec(memory_space=pltpu.VMEM),
        scratch_shapes=[
            pltpu.VMEM((2, 4, per_quarter, TILE), BF16),
            pltpu.VMEM((2, 4, per_quarter, TILE), BF16),
            pltpu.VMEM((2, 3, per_quarter, TILE), BF16),
            pltpu.VMEM((2, nb - 2, per_quarter, TILE), BF16),
            pltpu.VMEM((2, nb - 2, per_quarter, TILE), BF16),
            pltpu.VMEM((size_b, size_b), BF16),
            pltpu.VMEM((chunks, 3, *part), BF16),
            pltpu.VMEM((chunks, *part), BF16),
            pltpu.VMEM((chunks, nb - 2, *part), BF16),
            pltpu.VMEM((chunks, nb - 2, *part), BF16),
            pltpu.VMEM((2, size_b, size_b), F32),
            pltpu.VMEM((size_b, size_b), F32),
            pltpu.VMEM((8, TILE), F32),
            pltpu.VMEM((owners - 1, 8, TILE), F32),
            pltpu.SemaphoreType.DMA((2 + chunks, 4 + nb)),
            pltpu.SemaphoreType.DMA((2 + chunks, 4 + nb)),
            pltpu.SemaphoreType.DMA((owners - 1,)),
            pltpu.SemaphoreType.DMA((owners - 1,)),
        ],
        compiler_params=pltpu.CompilerParams(
            collective_id=0, has_side_effects=True, vmem_limit_bytes=48 * 1024 * 1024
        ),
    )(block_layer, gradients[0, 0])
    return out[None]


def solution(mesh):
    return jax.shard_map(
        functools.partial(per_device, mesh.shape["dp"], mesh.shape["owner"]),
        mesh=mesh,
        in_specs=(P("dp", "owner", None, None), P("owner")),
        out_specs=P("owner", "dp", None),
        check_vma=False,
    )
```

```python
import functools

import jax
import jax.numpy as jnp
from jax import lax
from jax.experimental import pallas as pl
from jax.experimental.pallas import tpu as pltpu
from jax.sharding import PartitionSpec as P

ITERS = 3
TILE = 128
EXTRA = 16
LEFT_ORDERS = ((0, 1), (1, 0))
RIGHT_ORDERS = ((0, 1), (1, 0))
GRAD_ORDERS = ((0, 1), (1, 0))
PROGRAM = "BAgDAB1CDAB0DCA0B1CBA1DC0ABllDlC1ll0MDCrrrrr"
BF16 = jnp.bfloat16
F32 = jnp.float32
MESH = pl.DeviceIdType.MESH


def mm(a, b):
    return jnp.dot(a.astype(BF16), b.astype(BF16), preferred_element_type=F32)


def iotas(rows, cols):
    return (
        lax.broadcasted_iota(jnp.int32, (rows, cols), 0),
        lax.broadcasted_iota(jnp.int32, (rows, cols), 1),
    )


def off_tiles(size_b):
    t = size_b // TILE
    return [(i, j) for i in range(t) for j in range(i + 1, t)]


def tile(array, i, j):
    return array[i * TILE:(i + 1) * TILE, j * TILE:(j + 1) * TILE]


def places(size_b, pieces):
    per_quarter = (size_b // TILE) ** 2 // 8 // pieces
    for p in range(pieces):
        for q in range(4):
            for k in range(per_quarter):
                yield p, q, slice(k * TILE, (k + 1) * TILE)


def quarter_rows(size_b, pieces):
    return size_b * size_b // (8 * pieces * TILE)


def pack(gram, acc_ref, size_b, pieces):
    t = size_b // TILE
    spots = places(size_b, pieces)
    row, col = iotas(TILE, TILE)
    sub, _ = iotas(EXTRA, TILE)
    extra = jnp.zeros((EXTRA, TILE), F32)
    for d in range(0, t, 2):
        second = tile(gram, d + 1, d + 1)
        acc_ref[next(spots)] = jnp.where(row <= col, tile(gram, d, d), second).astype(BF16)
        diagonal = jnp.sum(jnp.where(row == col, second, 0.0), axis=0, keepdims=True)
        extra = jnp.where(sub == d // 2, diagonal, extra)
    for (i, j), spot in zip(off_tiles(size_b), spots):
        acc_ref[spot] = tile(gram, i, j).astype(BF16)
    for q in range(4):
        value = extra if q == 0 else jnp.zeros((EXTRA, TILE), F32)
        acc_ref[0, q, quarter_rows(size_b, pieces):, :] = value.astype(BF16)


def unpack(gath_ref, stat_ref, size_b, pieces):
    t = size_b // TILE
    spots = places(size_b, pieces)
    row, col = iotas(TILE, TILE)
    extra = gath_ref[0, 0, quarter_rows(size_b, pieces):, :].astype(F32)
    for d in range(0, t, 2):
        both = gath_ref[next(spots)].astype(F32)
        turned = both.T
        first = jnp.where(row <= col, both, turned)
        second = jnp.where(row > col, both, turned)
        second = jnp.where(row == col, extra[d // 2:d // 2 + 1, :], second)
        for k, block in ((d, first), (d + 1, second)):
            stat_ref[k * TILE:(k + 1) * TILE, k * TILE:(k + 1) * TILE] = block
    for (i, j), spot in zip(off_tiles(size_b), spots):
        block = gath_ref[spot].astype(F32)
        stat_ref[i * TILE:(i + 1) * TILE, j * TILE:(j + 1) * TILE] = block
        stat_ref[j * TILE:(j + 1) * TILE, i * TILE:(i + 1) * TILE] = block.T


def solver(gath_ref, stat_ref, size_b, pieces, result):
    unpack(gath_ref, stat_ref, size_b, pieces)
    row, col = iotas(size_b, size_b)
    diag = row == col
    stat = stat_ref[...]
    trace = jnp.sum(jnp.where(diag, stat, 0.0), keepdims=True)
    ridge = 0.01 * trace / size_b + 1e-06
    shifted = stat + jnp.where(diag, ridge, 0.0)
    norm2 = jnp.sum(shifted * shifted, keepdims=True)
    m = shifted * lax.rsqrt(norm2)
    yield
    t = (mm(m, m) - 10.0 * m) * 0.0625
    once = 1.5625 * m + mm(m, t)
    yield
    nxt = 1.5625 * once + mm(t, once)
    a = 1.5625
    y = 0.0625 * mm(once, once) - 0.3125 * (m + nxt)
    for step in range(2, ITERS):
        m = nxt
        yield
        t = (mm(m, m) - 10.0 * m) * 0.0625
        yield
        once = 1.5625 * m + mm(m, t)
        part = 1.5625 * y + a * t + mm(y, t)
        if step + 1 < ITERS:
            nxt = 1.5625 * once + mm(t, once)
        y = 1.25 * y - 0.25 * (1.5625 * a * once + mm(part, once))
        a = 1.25 * a
    result["scale"] = lax.rsqrt(jnp.sqrt(jnp.sqrt(norm2)))
    result["a"], result["y"] = a, y.astype(BF16)


class Piece:
    def __init__(self, me, nb, order, src, land, forward, xsend, xland, gath, keep, send,
                 recv, target):
        self.me, self.nb, self.order = me, nb, order
        self.src, self.land, self.forward = src, land, forward
        self.xsend, self.xland, self.gath, self.keep = xsend, xland, gath, keep
        self.send, self.recv, self.target = send, recv, target
        self.mine = lax.rem(me, 4)
        self.flow = self.run()
        self.started = []

    def partner(self, mask):
        other = self.me
        for number in range(self.nb):
            if mask >> number & 1:
                other = other + (1 - 2 * (self.me // (1 << number) % 2)) * (1 << number)
        return other

    def copy(self, src, dst, slot, mask):
        copy = pltpu.make_async_remote_copy(
            src_ref=src,
            dst_ref=dst,
            send_sem=self.send.at[slot],
            recv_sem=self.recv.at[slot],
            device_id=self.target(self.partner(mask)),
            device_id_type=MESH,
        )
        copy.start()
        self.started.append(copy)
        return copy

    def run(self):
        low = lambda mask: lax.rem(self.partner(mask), 4)
        if self.order is None:
            copies = [
                self.copy(self.src(low(mask)), self.land.at[mask - 1], mask - 1, mask)
                for mask in (1, 2, 3)
            ]
            yield
            total = self.src(self.mine)[...].astype(F32)
            for n, copy in enumerate(copies):
                copy.wait_recv()
                total += self.land[n].astype(F32)
        else:
            first, second = (1 << bit for bit in self.order)
            onward = self.copy(self.src(low(3)), self.land.at[0], 0, first)
            stay = self.copy(self.src(low(first)), self.land.at[1], 1, first)
            yield
            onward.wait_recv()
            passing = self.src(low(second))[...].astype(F32) + self.land[0].astype(F32)
            self.forward[0] = passing.astype(BF16)
            last = self.copy(self.forward.at[0], self.land.at[2], 2, second)
            yield
            stay.wait_recv()
            total = self.src(self.mine)[...].astype(F32) + self.land[1].astype(F32)
            last.wait_recv()
            total += self.land[2].astype(F32)
        for n in range(self.nb - 2):
            self.xsend[n] = total.astype(BF16)
            copy = self.copy(self.xsend.at[n], self.xland.at[n], 6 + n, 4 << n)
            if n == 0:
                yield
            copy.wait_recv()
            total = self.xsend[n].astype(F32) + self.xland[n].astype(F32)
        if self.keep is not None:
            self.keep[...] = total.astype(BF16)
            return
        self.gath(self.mine)[...] = total.astype(BF16)
        own = self.gath(self.mine)
        if self.order is None:
            copies = [self.copy(own, own, 2 + mask, mask) for mask in (1, 2, 3)]
            yield
            for copy in copies:
                copy.wait_recv()
        else:
            near = self.copy(own, own, 3, second)
            far = self.copy(own, own, 4, first)
            yield
            near.wait_recv()
            other = self.gath(low(second))
            rest = self.copy(other, other, 5, first)
            yield
            far.wait_recv()
            rest.wait_recv()

    def attend(self):
        next(self.flow, None)


def kernel(dp_count, owners, layer_ref, g_ref, out_ref, *refs):
    bufs, (acc_l, acc_r, gath_l, gath_r, columns, summed, middle, arrived, stats, whole_ref,
           e_src, e_buf, send, recv, m_send, m_recv, e_send, e_recv) = refs[:-18], refs[-18:]
    me = lax.axis_index("dp")
    own = lax.axis_index("owner")
    size_b = g_ref.shape[0]
    nb = dp_count.bit_length() - 1
    height = out_ref.shape[0]
    quarter = size_b // 4
    depth = size_b // len(GRAD_ORDERS)

    target = lambda partner: (partner, own)
    pieces = {}

    def add(name, order, src, gath, keep):
        n = len(pieces)
        land, forward, xsend, xland = bufs[4 * n:4 * n + 4]
        pieces[name] = Piece(
            me, nb, order, src, land, forward, xsend, xland, gath, keep, send.at[n], recv.at[n],
            target,
        )

    for names, orders, acc, gath in (
        ("AB", LEFT_ORDERS, acc_l, gath_l), ("CD", RIGHT_ORDERS, acc_r, gath_r)
    ):
        for p, order in enumerate(orders):
            def block(ref, p=p, rows=quarter_rows(size_b, len(orders)) + (p == 0) * EXTRA):
                return lambda q: ref.at[p, q, :rows]
            add(names[p], order, block(acc), block(gath), None)
    for n, order in enumerate(GRAD_ORDERS):
        rows = slice(n * depth, (n + 1) * depth)
        add(str(n), order, lambda q, rows=rows: columns.at[q, rows], None, summed.at[rows])
    mine_low = lax.rem(me, 4)

    barrier = pltpu.get_barrier_semaphore()
    masks = [1, 2, 3] + [4 << n for n in range(nb - 2)]
    for mask in masks:
        peer = pieces["A"].partner(mask)
        pl.semaphore_signal(barrier, inc=1, device_id=(peer, own), device_id_type=MESH)
    for j in range(1, owners):
        pl.semaphore_signal(
            barrier, inc=1, device_id=(me, lax.rem(own + j, owners)), device_id_type=MESH
        )
    g = g_ref[...]
    for q in range(4):
        columns[q] = g[:, q * quarter:(q + 1) * quarter]
    pack(
        lax.dot_general(g, g, (((1,), (1,)), ((), ())), preferred_element_type=F32),
        acc_l, size_b, len(LEFT_ORDERS),
    )
    pl.semaphore_wait(barrier, len(masks) + owners - 1)

    left, right = {}, {}
    solves = {
        "l": solver(gath_l, stats.at[0], size_b, len(LEFT_ORDERS), left),
        "r": solver(gath_r, stats.at[1], size_b, len(RIGHT_ORDERS), right),
    }
    for token in PROGRAM:
        if token == "g":
            pack(
                lax.dot_general(g, g, (((0,), (0,)), ((), ())), preferred_element_type=F32),
                acc_r, size_b, len(RIGHT_ORDERS),
            )
        elif token in solves:
            next(solves[token], None)
        elif token == "M":
            grad = summed[...]
            value = left["scale"] * (left["a"] * grad.astype(F32) + mm(left["y"], grad))
            middle[...] = value.astype(BF16).reshape(middle.shape)
            moves = []
            for mask in (1, 2, 3):
                peer = pieces["A"].partner(mask)
                move = pltpu.make_async_remote_copy(
                    src_ref=middle.at[:, lax.rem(peer, 4)],
                    dst_ref=arrived.at[mine_low],
                    send_sem=m_send.at[mask - 1],
                    recv_sem=m_recv.at[mask - 1],
                    device_id=target(peer),
                    device_id_type=MESH,
                )
                move.start()
                moves.append(move)
            arrived[mine_low] = middle[:, mine_low]
        else:
            pieces[token].attend()
    for move in moves:
        move.wait_recv()
    ours = jnp.concatenate([arrived[q].reshape(quarter, quarter) for q in range(4)], axis=1)
    whole = right["a"] * ours.astype(F32) + mm(ours, right["y"])
    whole = (right["scale"] / dp_count) * whole
    whole_ref[...] = whole.reshape(whole_ref.shape)
    energy = jnp.sum(whole * whole, keepdims=True)

    layer = layer_ref[0]
    _, lane = iotas(*e_src.shape)
    of_energy = lane == layer
    of_count = lane == layer + TILE // 2
    e_src[...] = jnp.where(of_energy, energy, jnp.where(of_count, float(quarter * size_b), 0.0))
    copies = []
    for mask in range(4):
        for j in range(owners):
            if mask + j == 0:
                continue
            n = mask * owners + j - 1
            copy = pltpu.make_async_remote_copy(
                src_ref=e_src,
                dst_ref=e_buf.at[n],
                send_sem=e_send.at[n],
                recv_sem=e_recv.at[n],
                device_id=(pieces["A"].partner(mask), lax.rem(own + j, owners)),
                device_id_type=MESH,
            )
            copy.start()
            copies.append(copy)
    for copy in moves + [copy for piece in pieces.values() for copy in piece.started]:
        copy.wait_send()
    rows = whole_ref[me // 4]
    for copy in copies:
        copy.wait()
    totals = e_src[...]
    for n in range(len(copies)):
        totals += e_buf[n]
    energies = jnp.sum(jnp.where(of_energy, totals, 0.0), keepdims=True)
    counts = jnp.sum(jnp.where(of_count, totals, 0.0), keepdims=True)
    out_ref[...] = (rows * lax.rsqrt(energies / counts + 1e-06)).astype(BF16)


def per_device(dp_count, owners, gradients, block_layer):
    size_b = gradients.shape[-1]
    nb = dp_count.bit_length() - 1
    height = size_b // dp_count
    shapes, packed = [], []
    for orders in (LEFT_ORDERS, RIGHT_ORDERS):
        rows = quarter_rows(size_b, len(orders))
        packed.append(pltpu.VMEM((len(orders), 4, rows + EXTRA, TILE), BF16))
        shapes += [(rows + (p == 0) * EXTRA, TILE) for p in range(len(orders))]
    shapes += [(size_b // len(GRAD_ORDERS), size_b // 4)] * len(GRAD_ORDERS)
    bufs = []
    for part in shapes:
        bufs += [
            pltpu.VMEM((n, *part), BF16) for n in (3, 1, nb - 2, nb - 2)
        ]
    out = pl.pallas_call(
        functools.partial(kernel, dp_count, owners),
        out_shape=jax.ShapeDtypeStruct((height, size_b), BF16),
        in_specs=[
            pl.BlockSpec(memory_space=pltpu.SMEM),
            pl.BlockSpec(memory_space=pltpu.VMEM),
        ],
        out_specs=pl.BlockSpec(memory_space=pltpu.VMEM),
        scratch_shapes=[
            *bufs,
            *packed,
            *packed,
            pltpu.VMEM((4, size_b, size_b // 4), BF16),
            pltpu.VMEM((size_b, size_b // 4), BF16),
            pltpu.VMEM((dp_count // 4, 4, height, size_b // 4), BF16),
            pltpu.VMEM((4, dp_count // 4, height, size_b // 4), BF16),
            pltpu.VMEM((2, size_b, size_b), F32),
            pltpu.VMEM((dp_count // 4, height, size_b), F32),
            pltpu.VMEM((1, TILE), F32),
            pltpu.VMEM((4 * owners - 1, 1, TILE), F32),
            pltpu.SemaphoreType.DMA((len(shapes), 4 + nb)),
            pltpu.SemaphoreType.DMA((len(shapes), 4 + nb)),
            pltpu.SemaphoreType.DMA((3,)),
            pltpu.SemaphoreType.DMA((3,)),
            pltpu.SemaphoreType.DMA((4 * owners - 1,)),
            pltpu.SemaphoreType.DMA((4 * owners - 1,)),
        ],
        compiler_params=pltpu.CompilerParams(
            collective_id=0, has_side_effects=True, vmem_limit_bytes=48 * 1024 * 1024
        ),
    )(block_layer, gradients[0, 0])
    return out[None]


def solution(mesh):
    return jax.shard_map(
        functools.partial(per_device, mesh.shape["dp"], mesh.shape["owner"]),
        mesh=mesh,
        in_specs=(P("dp", "owner", None, None), P("owner")),
        out_specs=P("owner", "dp", None),
        check_vma=False,
    )
```

```python
import functools

import jax
import jax.numpy as jnp
from jax import lax
from jax.experimental import pallas as pl
from jax.experimental.pallas import tpu as pltpu
from jax.sharding import PartitionSpec as P

ITERS = 3
TILE = 128
EXTRA = 16
LEFT_ORDERS = ((0, 1), (1, 0))
RIGHT_ORDERS = ((0, 1), (1, 0))
GRAD_ORDERS = ((0, 1), (0, 1))
PROGRAM = "ABgDCAB1CADB01CAB0DABC1A0DBllCllD1l0MCDrrrrr"
BF16 = jnp.bfloat16
F32 = jnp.float32
MESH = pl.DeviceIdType.MESH


def mm(a, b):
    return jnp.dot(a.astype(BF16), b.astype(BF16), preferred_element_type=F32)


def iotas(rows, cols):
    return (
        lax.broadcasted_iota(jnp.int32, (rows, cols), 0),
        lax.broadcasted_iota(jnp.int32, (rows, cols), 1),
    )


def off_tiles(size_b):
    t = size_b // TILE
    return [(i, j) for i in range(t) for j in range(i + 1, t)]


def tile(array, i, j):
    return array[i * TILE:(i + 1) * TILE, j * TILE:(j + 1) * TILE]


def places(size_b, pieces):
    per_quarter = (size_b // TILE) ** 2 // 8 // pieces
    for p in range(pieces):
        for q in range(4):
            for k in range(per_quarter):
                yield p, q, slice(k * TILE, (k + 1) * TILE)


def quarter_rows(size_b, pieces):
    return size_b * size_b // (8 * pieces * TILE)


def pack(gram, acc_ref, size_b, pieces):
    t = size_b // TILE
    spots = places(size_b, pieces)
    row, col = iotas(TILE, TILE)
    sub, _ = iotas(EXTRA, TILE)
    extra = jnp.zeros((EXTRA, TILE), F32)
    for d in range(0, t, 2):
        second = tile(gram, d + 1, d + 1)
        acc_ref[next(spots)] = jnp.where(row <= col, tile(gram, d, d), second).astype(BF16)
        diagonal = jnp.sum(jnp.where(row == col, second, 0.0), axis=0, keepdims=True)
        extra = jnp.where(sub == d // 2, diagonal, extra)
    for (i, j), spot in zip(off_tiles(size_b), spots):
        acc_ref[spot] = tile(gram, i, j).astype(BF16)
    for q in range(4):
        value = extra if q == 0 else jnp.zeros((EXTRA, TILE), F32)
        acc_ref[0, q, quarter_rows(size_b, pieces):, :] = value.astype(BF16)


def unpack(gath_ref, stat_ref, size_b, pieces):
    t = size_b // TILE
    spots = places(size_b, pieces)
    row, col = iotas(TILE, TILE)
    extra = gath_ref[0, 0, quarter_rows(size_b, pieces):, :].astype(F32)
    for d in range(0, t, 2):
        both = gath_ref[next(spots)].astype(F32)
        turned = both.T
        first = jnp.where(row <= col, both, turned)
        second = jnp.where(row > col, both, turned)
        second = jnp.where(row == col, extra[d // 2:d // 2 + 1, :], second)
        for k, block in ((d, first), (d + 1, second)):
            stat_ref[k * TILE:(k + 1) * TILE, k * TILE:(k + 1) * TILE] = block
    for (i, j), spot in zip(off_tiles(size_b), spots):
        block = gath_ref[spot].astype(F32)
        stat_ref[i * TILE:(i + 1) * TILE, j * TILE:(j + 1) * TILE] = block
        stat_ref[j * TILE:(j + 1) * TILE, i * TILE:(i + 1) * TILE] = block.T


def solver(gath_ref, stat_ref, size_b, pieces, result):
    unpack(gath_ref, stat_ref, size_b, pieces)
    row, col = iotas(size_b, size_b)
    diag = row == col
    stat = stat_ref[...]
    trace = jnp.sum(jnp.where(diag, stat, 0.0), keepdims=True)
    ridge = 0.01 * trace / size_b + 1e-06
    shifted = stat + jnp.where(diag, ridge, 0.0)
    norm2 = jnp.sum(shifted * shifted, keepdims=True)
    m = shifted * lax.rsqrt(norm2)
    yield
    t = (mm(m, m) - 10.0 * m) * 0.0625
    once = 1.5625 * m + mm(m, t)
    yield
    nxt = 1.5625 * once + mm(t, once)
    a = 1.5625
    y = 0.0625 * mm(once, once) - 0.3125 * (m + nxt)
    for step in range(2, ITERS):
        m = nxt
        yield
        t = (mm(m, m) - 10.0 * m) * 0.0625
        yield
        once = 1.5625 * m + mm(m, t)
        part = 1.5625 * y + a * t + mm(y, t)
        if step + 1 < ITERS:
            nxt = 1.5625 * once + mm(t, once)
        y = 1.25 * y - 0.25 * (1.5625 * a * once + mm(part, once))
        a = 1.25 * a
    result["scale"] = lax.rsqrt(jnp.sqrt(jnp.sqrt(norm2)))
    result["a"], result["y"] = a, y.astype(BF16)


class Piece:
    def __init__(self, me, nb, order, src, land, forward, xsend, xland, gath, keep, send,
                 recv, target):
        self.me, self.nb, self.order = me, nb, order
        self.src, self.land, self.forward = src, land, forward
        self.xsend, self.xland, self.gath, self.keep = xsend, xland, gath, keep
        self.send, self.recv, self.target = send, recv, target
        self.mine = lax.rem(me, 4)
        self.flow = self.run()
        self.started = []

    def partner(self, mask):
        other = self.me
        for number in range(self.nb):
            if mask >> number & 1:
                other = other + (1 - 2 * (self.me // (1 << number) % 2)) * (1 << number)
        return other

    def copy(self, src, dst, slot, mask):
        copy = pltpu.make_async_remote_copy(
            src_ref=src,
            dst_ref=dst,
            send_sem=self.send.at[slot],
            recv_sem=self.recv.at[slot],
            device_id=self.target(self.partner(mask)),
            device_id_type=MESH,
        )
        copy.start()
        self.started.append(copy)
        return copy

    def run(self):
        low = lambda mask: lax.rem(self.partner(mask), 4)
        if self.order is None:
            copies = [
                self.copy(self.src(low(mask)), self.land.at[mask - 1], mask - 1, mask)
                for mask in (1, 2, 3)
            ]
            yield
            total = self.src(self.mine)[...].astype(F32)
            for n, copy in enumerate(copies):
                copy.wait_recv()
                total += self.land[n].astype(F32)
        else:
            first, second = (1 << bit for bit in self.order)
            onward = self.copy(self.src(low(3)), self.land.at[0], 0, first)
            stay = self.copy(self.src(low(first)), self.land.at[1], 1, first)
            yield
            onward.wait_recv()
            passing = self.src(low(second))[...].astype(F32) + self.land[0].astype(F32)
            self.forward[0] = passing.astype(BF16)
            last = self.copy(self.forward.at[0], self.land.at[2], 2, second)
            yield
            stay.wait_recv()
            total = self.src(self.mine)[...].astype(F32) + self.land[1].astype(F32)
            last.wait_recv()
            total += self.land[2].astype(F32)
        for n in range(self.nb - 2):
            self.xsend[n] = total.astype(BF16)
            copy = self.copy(self.xsend.at[n], self.xland.at[n], 6 + n, 4 << n)
            if n == 0:
                yield
            copy.wait_recv()
            total = self.xsend[n].astype(F32) + self.xland[n].astype(F32)
        if self.keep is not None:
            self.keep[...] = total.astype(BF16)
            return
        self.gath(self.mine)[...] = total.astype(BF16)
        own = self.gath(self.mine)
        if self.order is None:
            copies = [self.copy(own, own, 2 + mask, mask) for mask in (1, 2, 3)]
            yield
            for copy in copies:
                copy.wait_recv()
        else:
            near = self.copy(own, own, 3, second)
            far = self.copy(own, own, 4, first)
            yield
            near.wait_recv()
            other = self.gath(low(second))
            rest = self.copy(other, other, 5, first)
            yield
            far.wait_recv()
            rest.wait_recv()

    def attend(self):
        next(self.flow, None)


def kernel(dp_count, owners, layer_ref, g_ref, out_ref, *refs):
    bufs, (acc_l, acc_r, gath_l, gath_r, columns, summed, middle, arrived, stats, whole_ref,
           e_src, e_buf, send, recv, m_send, m_recv, e_send, e_recv) = refs[:-18], refs[-18:]
    me = lax.axis_index("dp")
    own = lax.axis_index("owner")
    size_b = g_ref.shape[0]
    nb = dp_count.bit_length() - 1
    height = out_ref.shape[0]
    quarter = size_b // 4
    depth = size_b // len(GRAD_ORDERS)

    target = lambda partner: (partner, own)
    pieces = {}

    def add(name, order, src, gath, keep):
        n = len(pieces)
        land, forward, xsend, xland = bufs[4 * n:4 * n + 4]
        pieces[name] = Piece(
            me, nb, order, src, land, forward, xsend, xland, gath, keep, send.at[n], recv.at[n],
            target,
        )

    for names, orders, acc, gath in (
        ("AB", LEFT_ORDERS, acc_l, gath_l), ("CD", RIGHT_ORDERS, acc_r, gath_r)
    ):
        for p, order in enumerate(orders):
            def block(ref, p=p, rows=quarter_rows(size_b, len(orders)) + (p == 0) * EXTRA):
                return lambda q: ref.at[p, q, :rows]
            add(names[p], order, block(acc), block(gath), None)
    for n, order in enumerate(GRAD_ORDERS):
        rows = slice(n * depth, (n + 1) * depth)
        add(str(n), order, lambda q, rows=rows: columns.at[q, rows], None, summed.at[rows])
    mine_low = lax.rem(me, 4)

    barrier = pltpu.get_barrier_semaphore()
    masks = [1, 2, 3] + [4 << n for n in range(nb - 2)]
    for mask in masks:
        peer = pieces["A"].partner(mask)
        pl.semaphore_signal(barrier, inc=1, device_id=(peer, own), device_id_type=MESH)
    for j in range(1, owners):
        pl.semaphore_signal(
            barrier, inc=1, device_id=(me, lax.rem(own + j, owners)), device_id_type=MESH
        )
    g = g_ref[...]
    for q in range(4):
        columns[q] = g[:, q * quarter:(q + 1) * quarter]
    pack(
        lax.dot_general(g, g, (((1,), (1,)), ((), ())), preferred_element_type=F32),
        acc_l, size_b, len(LEFT_ORDERS),
    )
    pl.semaphore_wait(barrier, len(masks) + owners - 1)

    left, right = {}, {}
    solves = {
        "l": solver(gath_l, stats.at[0], size_b, len(LEFT_ORDERS), left),
        "r": solver(gath_r, stats.at[1], size_b, len(RIGHT_ORDERS), right),
    }
    for token in PROGRAM:
        if token == "g":
            pack(
                lax.dot_general(g, g, (((0,), (0,)), ((), ())), preferred_element_type=F32),
                acc_r, size_b, len(RIGHT_ORDERS),
            )
        elif token in solves:
            next(solves[token], None)
        elif token == "M":
            grad = summed[...]
            value = left["scale"] * (left["a"] * grad.astype(F32) + mm(left["y"], grad))
            middle[...] = value.astype(BF16).reshape(middle.shape)
            moves = []
            for mask in (1, 2, 3):
                peer = pieces["A"].partner(mask)
                move = pltpu.make_async_remote_copy(
                    src_ref=middle.at[:, lax.rem(peer, 4)],
                    dst_ref=arrived.at[mine_low],
                    send_sem=m_send.at[mask - 1],
                    recv_sem=m_recv.at[mask - 1],
                    device_id=target(peer),
                    device_id_type=MESH,
                )
                move.start()
                moves.append(move)
            arrived[mine_low] = middle[:, mine_low]
        else:
            pieces[token].attend()
    for move in moves:
        move.wait_recv()
    ours = jnp.concatenate([arrived[q].reshape(quarter, quarter) for q in range(4)], axis=1)
    whole = right["a"] * ours.astype(F32) + mm(ours, right["y"])
    whole = (right["scale"] / dp_count) * whole
    whole_ref[...] = whole.reshape(whole_ref.shape)
    energy = jnp.sum(whole * whole, keepdims=True)

    layer = layer_ref[0]
    _, lane = iotas(*e_src.shape)
    of_energy = lane == layer
    of_count = lane == layer + TILE // 2
    e_src[...] = jnp.where(of_energy, energy, jnp.where(of_count, float(quarter * size_b), 0.0))
    copies = []
    for mask in (3, 2, 1, 0):
        for j in range(owners):
            if mask + j == 0:
                continue
            n = mask * owners + j - 1
            copy = pltpu.make_async_remote_copy(
                src_ref=e_src,
                dst_ref=e_buf.at[n],
                send_sem=e_send.at[n],
                recv_sem=e_recv.at[n],
                device_id=(pieces["A"].partner(mask), lax.rem(own + j, owners)),
                device_id_type=MESH,
            )
            copy.start()
            copies.append(copy)
    rows = whole_ref[me // 4]
    for copy in copies:
        copy.wait_recv()
    totals = e_src[...]
    for n in range(len(copies)):
        totals += e_buf[n]
    energies = jnp.sum(jnp.where(of_energy, totals, 0.0), keepdims=True)
    counts = jnp.sum(jnp.where(of_count, totals, 0.0), keepdims=True)
    out_ref[...] = (rows * lax.rsqrt(energies / counts + 1e-06)).astype(BF16)
    started = [copy for piece in pieces.values() for copy in piece.started]
    for copy in started + moves + copies:
        copy.wait_send()


def per_device(dp_count, owners, gradients, block_layer):
    size_b = gradients.shape[-1]
    nb = dp_count.bit_length() - 1
    height = size_b // dp_count
    shapes, packed = [], []
    for orders in (LEFT_ORDERS, RIGHT_ORDERS):
        rows = quarter_rows(size_b, len(orders))
        packed.append(pltpu.VMEM((len(orders), 4, rows + EXTRA, TILE), BF16))
        shapes += [(rows + (p == 0) * EXTRA, TILE) for p in range(len(orders))]
    shapes += [(size_b // len(GRAD_ORDERS), size_b // 4)] * len(GRAD_ORDERS)
    bufs = []
    for part in shapes:
        bufs += [
            pltpu.VMEM((n, *part), BF16) for n in (3, 1, nb - 2, nb - 2)
        ]
    out = pl.pallas_call(
        functools.partial(kernel, dp_count, owners),
        out_shape=jax.ShapeDtypeStruct((height, size_b), BF16),
        in_specs=[
            pl.BlockSpec(memory_space=pltpu.SMEM),
            pl.BlockSpec(memory_space=pltpu.VMEM),
        ],
        out_specs=pl.BlockSpec(memory_space=pltpu.VMEM),
        scratch_shapes=[
            *bufs,
            *packed,
            *packed,
            pltpu.VMEM((4, size_b, size_b // 4), BF16),
            pltpu.VMEM((size_b, size_b // 4), BF16),
            pltpu.VMEM((dp_count // 4, 4, height, size_b // 4), BF16),
            pltpu.VMEM((4, dp_count // 4, height, size_b // 4), BF16),
            pltpu.VMEM((2, size_b, size_b), F32),
            pltpu.VMEM((dp_count // 4, height, size_b), F32),
            pltpu.VMEM((1, TILE), F32),
            pltpu.VMEM((4 * owners - 1, 1, TILE), F32),
            pltpu.SemaphoreType.DMA((len(shapes), 4 + nb)),
            pltpu.SemaphoreType.DMA((len(shapes), 4 + nb)),
            pltpu.SemaphoreType.DMA((3,)),
            pltpu.SemaphoreType.DMA((3,)),
            pltpu.SemaphoreType.DMA((4 * owners - 1,)),
            pltpu.SemaphoreType.DMA((4 * owners - 1,)),
        ],
        compiler_params=pltpu.CompilerParams(
            collective_id=0, has_side_effects=True, vmem_limit_bytes=48 * 1024 * 1024
        ),
    )(block_layer, gradients[0, 0])
    return out[None]


def solution(mesh):
    return jax.shard_map(
        functools.partial(per_device, mesh.shape["dp"], mesh.shape["owner"]),
        mesh=mesh,
        in_specs=(P("dp", "owner", None, None), P("owner")),
        out_specs=P("owner", "dp", None),
        check_vma=False,
    )
```
